32 devices in a mesh: seq: 8 (over y, x, core), tensor: 4 (over z).
Axes of the slice: x: 2, y: 2, z: 4, core: 2. Of those that a mesh axis runs over, the one named last changes fastest.
Arguments:
- queries: bfloat16 [1024, 4096], P(('seq', 'tensor')), may hold values from -5 to 5
- keys: bfloat16 [1024, 1024], P(('seq', 'tensor')), may hold values from -5 to 5
- values: bfloat16 [1024, 1024], P(('seq', 'tensor')), may hold values from -5 to 5
- mamba_x: bfloat16 [1024, 8192], P(('seq', 'tensor')), may hold values from -5 to 5
- mamba_b: bfloat16 [1024, 1024], P(('seq', 'tensor')), may hold values from -5 to 5
- mamba_c: bfloat16 [1024, 1024], P(('seq', 'tensor')), may hold values from -5 to 5
- mamba_dt: bfloat16 [1024, 128], P(('seq', 'tensor')), may hold values from -4 to 4
- conv_x: bfloat16 [4, 8192], P(None, 'tensor'), may hold values from -3 to 3
- conv_b: bfloat16 [4, 1024], P(None, 'tensor'), may hold values from -3 to 3
- conv_c: bfloat16 [4, 1024], P(None, 'tensor'), may hold values from -3 to 3
- dt_bias: float32 [128], P('tensor'), may hold values from -1 to 1
- decay_rate: float32 [128], P('tensor'), may hold values from 0.0001 to 0.05
- skip_gain: float32 [128], P('tensor'), may hold values from 0.5 to 1.5
- norm_gain: float32 [8192], P('tensor'), may hold values from 0.5 to 1.5
- windows: int32 [32], replicated, may hold values from 160 to 640, as said below
- doc_lengths: int32 [3], replicated, may hold values from 1 to 768, 1024 in all
Outputs:
- attn_out: bfloat16 [1024, 4096], P('seq', 'tensor')
- mamba_out: bfloat16 [1024, 8192], P('seq', 'tensor')
- attn_checksum: float32 [4096], P('tensor')
- mamba_checksum: float32 [8192], P('tensor')
The draws below stay inside these ranges and needn't reach their ends.
Inputs may be any that keep to these rules, and one draw needn't show every extreme that they name: `windows`: one of the 32 query heads has a window of exactly 640 tokens. `doc_lengths`: 3 lengths summing to 1024; the longest is exactly three quarters of 1024.
All inputs are finite; a program needn't handle non-finite values.
Results may differ from the reference program's by a relative error of at most 0.007.
Values may be sent and summed in bfloat16 or wider, within the bound.
A program may use at most 192 MiB of HBM per device.

```python
import math
import jax
import jax.numpy as jnp
import numpy as np
from jax import lax

QUERY_HEAD_COUNT = 32
KEY_VALUE_HEADS = 8
HEAD_SIZE = 128
MH = 128
MP = 64
MN = 128
MG = 8
KC = 4
NDOC = 3
TOKENS_PER_INDEX = 128
SEQUENCE_LENGTH = 1024
LONGEST_WINDOW = 640


def keys_common(key):
    starting_key = jax.random.fold_in(key, 101)
    unscaled_keys = jnp.clip(jax.random.normal(starting_key, (SEQUENCE_LENGTH, KEY_VALUE_HEADS * HEAD_SIZE), jnp.float32), -5.0, 5.0)
    return unscaled_keys


def draw_keys(key, part):
    return keys_common(key).astype(jnp.bfloat16)


def draw_queries(key, part):
    drawn_rows = jnp.clip(jax.random.normal(jax.random.fold_in(key, 202), (SEQUENCE_LENGTH, QUERY_HEAD_COUNT * HEAD_SIZE), jnp.float32), -5.0, 5.0)
    return drawn_rows.astype(jnp.bfloat16)


def draw_windows(key, part):
    widths = jax.random.randint(jax.random.fold_in(key, 303), (QUERY_HEAD_COUNT,), LONGEST_WINDOW // 4, LONGEST_WINDOW + 1)
    chosen = jax.random.randint(jax.random.fold_in(key, 304), (), 0, QUERY_HEAD_COUNT)
    return jnp.where(jnp.arange(QUERY_HEAD_COUNT) == chosen, LONGEST_WINDOW, widths).astype(jnp.int32)


def block_levels(own_key, shape, split, least, top_value):
    loudness = 1.0
    for axis_at, shards_of in split:
        steps = jax.random.uniform(jax.random.fold_in(jax.random.fold_in(own_key, 6), axis_at), (shards_of,), jnp.float32, least / len(split), top_value / len(split))
        loudness = loudness * jnp.repeat(jnp.exp(steps), shape[axis_at] // shards_of).reshape((-1,) + (1,) * (len(shape) - 1 - axis_at))
    return loudness


def profile(number_of, total, most, lean):
    loads = [(1 << 20) // math.isqrt(grade ** lean) + 1 for grade in range(2, number_of + 1)]
    spare, counts = total - most - (number_of - 1), [1] * (number_of - 1)
    while spare > 0:
        movable = [i for i in range(number_of - 1) if counts[i] < most]
        mass, left = sum([loads[i] for i in movable]), spare
        for i in movable:
            more = min(most - counts[i], max(1, left * loads[i] // mass), spare)
            counts[i] = counts[i] + more
            spare = spare - more
    return np.array([most] + counts)


def ragged_sizes(key, amount, total, most, skew):
    if amount == 2:
        one = jax.random.randint(key, (), max(1, total - most), min(most, total - 1) + 1)
        return jnp.stack([one, total - one])
    lengths = jnp.asarray(profile(amount, total, most, skew), jnp.int32)
    couples = (amount - 1) // 2
    giver, taker = lengths[1:1 + 2 * couples:2], lengths[2:2 + 2 * couples:2]
    slack = jnp.minimum(giver - 1, most - taker)
    shifted = jax.random.randint(jax.random.fold_in(key, 1), (couples,), 0, 1 << 20) % (slack + 1)
    lengths = lengths.at[1:1 + 2 * couples:2].set(giver - shifted).at[2:2 + 2 * couples:2].set(taker + shifted)
    return lengths[jax.random.permutation(jax.random.fold_in(key, 2), amount)]


def noise(own_key, shape, width, reach, cuts=(), kind=jnp.bfloat16):
    loudness = block_levels(own_key, shape, cuts, -0.22, 0.18) if cuts else 1.0
    result = jax.random.normal(own_key, shape, jnp.float32) * width * loudness
    return jnp.minimum(jnp.maximum(result, -reach), reach).astype(kind)


def setup_inputs(seed: int = 0) -> dict:
    splits = jax.random.split(jax.random.key(seed), 17)
    return {
        "queries": draw_queries(jax.random.fold_in(splits[16], 71), 0),
        "keys": draw_keys(jax.random.fold_in(splits[16], 71), 0),
        "values": noise(splits[2], (SEQUENCE_LENGTH, KEY_VALUE_HEADS * HEAD_SIZE), 1.0, 5.0, ((0, 32),)),
        "mamba_x": noise(splits[3], (SEQUENCE_LENGTH, MH * MP), 1.0, 5.0, ((0, 32),)),
        "mamba_b": noise(splits[4], (SEQUENCE_LENGTH, MG * MN), 1.0, 5.0, ((0, 32),)),
        "mamba_c": noise(splits[5], (SEQUENCE_LENGTH, MG * MN), 1.0, 5.0, ((0, 32),)),
        "mamba_dt": noise(splits[6], (SEQUENCE_LENGTH, MH), 1.0, 4.0, ((0, 32),)),
        "conv_x": noise(splits[7], (KC, MH * MP), KC ** -0.5, 3.0, ((1, 4),)),
        "conv_b": noise(splits[8], (KC, MG * MN), KC ** -0.5, 3.0, ((1, 4),)),
        "conv_c": noise(splits[9], (KC, MG * MN), KC ** -0.5, 3.0, ((1, 4),)),
        "dt_bias": jnp.clip(jax.random.uniform(splits[10], (MH,), jnp.float32, -1.0, 1.0) * block_levels(splits[10], (MH,), ((0, 4),), -0.4, 0.0), -1.0, 1.0),
        "decay_rate": jnp.clip(jnp.exp(math.log(0.05) - 6.214608 * jax.random.uniform(splits[11], (MH,), jnp.float32) ** block_levels(splits[11], (MH,), ((0, 4),), -0.2, 0.2)), 0.0001, 0.05),
        "skip_gain": jnp.clip(0.5 + 1.0 * jax.random.uniform(splits[12], (MH,), jnp.float32) ** block_levels(splits[12], (MH,), ((0, 4),), -0.2, 0.2), 0.5, 1.5),
        "norm_gain": jnp.clip(1.0 + 0.1 * jax.random.normal(splits[13], (MH * MP,), jnp.float32), 0.5, 1.5),
        "windows": draw_windows(jax.random.fold_in(splits[16], 71), 0),
        "doc_lengths": ragged_sizes(splits[15], NDOC, SEQUENCE_LENGTH, 3 * SEQUENCE_LENGTH // 4, 1).astype(jnp.int32),
    }


NEG_LARGE = -1e+30
EPS_NORM = 1e-05

def doc_table(doc_lengths):
    return (jnp.cumsum(doc_lengths) - doc_lengths).astype(jnp.int32)

def doc_index(positions, doc_starts):
    return lax.optimization_barrier(jnp.sum((positions[:, None] >= doc_starts[None, :]).astype(jnp.int32), axis=1)) - 1

def allowed_mask(query_pos, key_pos, doc_starts, window_per_head):
    gap = query_pos[:, None] - key_pos[None, :]
    same_doc = doc_index(query_pos, doc_starts)[:, None] == doc_index(key_pos, doc_starts)[None, :]
    base_ok = (gap >= 0) & (key_pos[None, :] >= 0) & same_doc
    return base_ok[None, None] & (gap[None, None] < window_per_head[:, :, None, None])

def reference_attention(queries, keys, values, windows, doc_starts):
    group_width = QUERY_HEAD_COUNT // KEY_VALUE_HEADS
    window_per_head = windows.reshape(KEY_VALUE_HEADS, group_width)
    block_count = SEQUENCE_LENGTH // TOKENS_PER_INDEX
    padded_keys = jnp.pad(keys, ((LONGEST_WINDOW, 0), (0, 0)))
    padded_values = jnp.pad(values, ((LONGEST_WINDOW, 0), (0, 0)))

    def one_block(index):
        first = (index * TOKENS_PER_INDEX).astype(jnp.int32)
        query_tile_block = lax.dynamic_slice_in_dim(queries, first, TOKENS_PER_INDEX, 0)
        key_tile_block = lax.dynamic_slice_in_dim(padded_keys, first, LONGEST_WINDOW + TOKENS_PER_INDEX, 0)
        value_tile_block = lax.dynamic_slice_in_dim(padded_values, first, LONGEST_WINDOW + TOKENS_PER_INDEX, 0)
        query_pos = first + jnp.arange(TOKENS_PER_INDEX, dtype=jnp.int32)
        key_pos = first - LONGEST_WINDOW + jnp.arange(LONGEST_WINDOW + TOKENS_PER_INDEX, dtype=jnp.int32)
        grouped_heads = query_tile_block.reshape(TOKENS_PER_INDEX, KEY_VALUE_HEADS, group_width, HEAD_SIZE).astype(jnp.float32)
        keys_rank3 = key_tile_block.reshape(LONGEST_WINDOW + TOKENS_PER_INDEX, KEY_VALUE_HEADS, HEAD_SIZE).astype(jnp.float32)
        values_rank3 = value_tile_block.reshape(LONGEST_WINDOW + TOKENS_PER_INDEX, KEY_VALUE_HEADS, HEAD_SIZE).astype(jnp.float32)
        scores = jnp.einsum('tgqd,sgd->gqts', grouped_heads, keys_rank3) * (1.0 / math.sqrt(HEAD_SIZE))
        allowed = allowed_mask(query_pos, key_pos, doc_starts, window_per_head)
        scores = jnp.where(allowed, scores, NEG_LARGE)
        top_score = lax.optimization_barrier(jnp.max(scores, axis=-1, keepdims=True))
        weights = jnp.where(allowed, jnp.exp(scores - top_score), 0.0)
        totals = lax.optimization_barrier(jnp.sum(weights, axis=-1))
        rounded = weights.astype(jnp.bfloat16).astype(jnp.float32)
        mixed = jnp.einsum('gqts,sgd->gqtd', rounded, values_rank3)
        output = mixed / totals[..., None]
        return output.transpose(2, 0, 1, 3).reshape(TOKENS_PER_INDEX, QUERY_HEAD_COUNT * HEAD_SIZE).astype(jnp.bfloat16)
    blocks = lax.map(one_block, jnp.arange(block_count, dtype=jnp.int32))
    return blocks.reshape(SEQUENCE_LENGTH, QUERY_HEAD_COUNT * HEAD_SIZE)

def causal_conv(extended, taps, positions, doc_starts):
    count = positions.shape[0]
    docs_out = doc_index(positions, doc_starts)
    ext_pos = positions[0] - (KC - 1) + jnp.arange(count + KC - 1, dtype=jnp.int32)
    docs_ext = doc_index(ext_pos, doc_starts)
    running = jnp.zeros((count, extended.shape[1]), jnp.float32)
    for tap_index in range(KC):
        offset = KC - 1 - tap_index
        valid = (docs_ext[offset:offset + count] == docs_out) & (ext_pos[offset:offset + count] >= 0)
        term = taps[tap_index].astype(jnp.float32)[None, :] * extended[offset:offset + count].astype(jnp.float32)
        running = running + jnp.where(valid[:, None], term, 0.0)
    return jax.nn.silu(running).astype(jnp.bfloat16)

def stretch_terms(x_rows, b_rows, c_rows, dt_rows, positions, doc_starts, dt_bias, decay_rate):
    count = positions.shape[0]
    heads = x_rows.shape[1] // MP
    groups = b_rows.shape[1] // MN
    per_group = heads // groups
    docs = doc_index(positions, doc_starts)
    prior_doc = doc_index(positions[:1] - 1, doc_starts)[0]
    delta = jax.nn.softplus(dt_rows.astype(jnp.float32) + dt_bias[None, :])
    log_decay = -delta * decay_rate[None, :]
    running = jnp.cumsum(log_decay, axis=0)
    running_heads = running.T
    order = jnp.arange(count, dtype=jnp.int32)
    causal = order[:, None] >= order[None, :]
    same_doc = docs[:, None] == docs[None, :]
    gaps = running_heads[:, :, None] - running_heads[:, None, :]
    segment = jnp.where((causal & same_doc)[None], jnp.exp(jnp.minimum(gaps, 0.0)), 0.0)
    inputs3 = x_rows.reshape(count, heads, MP)
    b_groups = b_rows.reshape(count, groups, MN)
    c_groups = c_rows.reshape(count, groups, MN)
    cross = jnp.einsum('tgn,sgn->gts', c_groups.astype(jnp.float32), b_groups.astype(jnp.float32))
    cross_heads = jnp.repeat(cross, per_group, axis=0)
    mixing = (segment * cross_heads * delta.T[:, None, :]).astype(jnp.bfloat16)
    intra = jnp.einsum('hts,shp->thp', mixing.astype(jnp.float32), inputs3.astype(jnp.float32))
    last_doc = docs[count - 1]
    to_end = jnp.where((docs == last_doc)[:, None], jnp.exp(running[count - 1][None, :] - running), 0.0) * delta
    weighted = (inputs3.astype(jnp.float32) * to_end[:, :, None]).astype(jnp.bfloat16)
    b_heads = jnp.repeat(b_groups, per_group, axis=1)
    local_state = jnp.einsum('shp,shn->hpn', weighted.astype(jnp.float32), b_heads.astype(jnp.float32))
    carry_factor = jnp.where(prior_doc == last_doc, jnp.exp(running[count - 1]), 0.0)
    inflow = jnp.where((docs == prior_doc)[:, None], jnp.exp(running), 0.0)
    c_heads = jnp.repeat(c_groups, per_group, axis=1)
    return (intra, local_state, carry_factor, inflow, c_heads)

def stretch_finish(intra, incoming, inflow, c_heads, x_rows, skip_gain, norm_gain):
    count = x_rows.shape[0]
    heads = x_rows.shape[1] // MP
    incoming_bf = incoming.astype(jnp.bfloat16)
    entering = jnp.einsum('thn,hpn->thp', c_heads.astype(jnp.float32), incoming_bf.astype(jnp.float32)) * inflow[:, :, None]
    inputs3 = x_rows.reshape(count, heads, MP).astype(jnp.float32)
    mixed = intra + entering + skip_gain[None, :, None] * inputs3
    mean_square = lax.optimization_barrier(jnp.mean(mixed * mixed, axis=-1, keepdims=True))
    normed = mixed * lax.rsqrt(mean_square + EPS_NORM) * norm_gain.reshape(heads, MP)[None]
    return normed.reshape(count, heads * MP).astype(jnp.bfloat16)

def reference(queries, keys, values, mamba_x, mamba_b, mamba_c, mamba_dt, conv_x, conv_b, conv_c, dt_bias, decay_rate, skip_gain, norm_gain, windows, doc_lengths):
    doc_starts = doc_table(doc_lengths)
    attention = reference_attention(queries, keys, values, windows, doc_starts)
    positions = jnp.arange(SEQUENCE_LENGTH, dtype=jnp.int32)
    pad_rows = ((KC - 1, 0), (0, 0))
    conv_x_out = causal_conv(jnp.pad(mamba_x, pad_rows), conv_x, positions, doc_starts)
    conv_b_out = causal_conv(jnp.pad(mamba_b, pad_rows), conv_b, positions, doc_starts)
    conv_c_out = causal_conv(jnp.pad(mamba_c, pad_rows), conv_c, positions, doc_starts)
    stretch_count = SEQUENCE_LENGTH // TOKENS_PER_INDEX

    def stretch_step(incoming, inputs):
        index, x_rows, b_rows, c_rows, dt_rows = inputs
        stretch_pos = index * TOKENS_PER_INDEX + jnp.arange(TOKENS_PER_INDEX, dtype=jnp.int32)
        intra, local_state, carry_factor, inflow, c_heads = stretch_terms(x_rows, b_rows, c_rows, dt_rows, stretch_pos, doc_starts, dt_bias, decay_rate)
        output = stretch_finish(intra, incoming, inflow, c_heads, x_rows, skip_gain, norm_gain)
        updated = carry_factor[:, None, None] * incoming + local_state
        return (updated, output)
    initial = jnp.zeros((MH, MP, MN), jnp.float32)
    scanned = (jnp.arange(stretch_count, dtype=jnp.int32), conv_x_out.reshape(stretch_count, TOKENS_PER_INDEX, MH * MP), conv_b_out.reshape(stretch_count, TOKENS_PER_INDEX, MG * MN), conv_c_out.reshape(stretch_count, TOKENS_PER_INDEX, MG * MN), mamba_dt.reshape(stretch_count, TOKENS_PER_INDEX, MH))
    final_state, outputs = lax.scan(stretch_step, initial, scanned)
    mamba_out = outputs.reshape(SEQUENCE_LENGTH, MH * MP)
    return (attention, mamba_out, lax.optimization_barrier(jnp.sum(attention.astype(jnp.float32), axis=0)), lax.optimization_barrier(jnp.sum(mamba_out.astype(jnp.float32), axis=0)))
```

```python
import functools
import math

import jax
import jax.numpy as jnp
from jax import lax
from jax.experimental import pallas as pl
from jax.experimental.pallas import tpu as pltpu
from jax.sharding import PartitionSpec as P

HEAD_SIZE = 128
MP = 64
MN = 128
KC = 4
TAIL = 16
LANES = 128

NEG_LARGE = -1e30
EPS_NORM = 1e-05
F32 = jnp.float32
BF16 = jnp.bfloat16


def parts3(v):
    a = v.astype(BF16)
    r = v - a.astype(F32)
    b = r.astype(BF16)
    c = (r - b.astype(F32)).astype(BF16)
    return a, b, c


def mm(a, b):
    return jnp.dot(a, b, preferred_element_type=F32)


def mm_t(a, b):
    return lax.dot_general(a, b, (((1,), (1,)), ((), ())), preferred_element_type=F32)


def iota(shape, dim):
    return lax.broadcasted_iota(jnp.int32, shape, dim)


def doc_of(pos, starts):
    total = jnp.full(pos.shape, -1, jnp.int32)
    for s in starts:
        total = total + (pos >= s).astype(jnp.int32)
    return total


def rdma(src, dst, send, recv, axis, peer):
    return pltpu.make_async_remote_copy(
        src_ref=src,
        dst_ref=dst,
        send_sem=send,
        recv_sem=recv,
        device_id={axis: peer},
        device_id_type=pl.DeviceIdType.MESH,
    )


def kernel(
    S,
    T,
    q_in,
    k_in,
    v_in,
    x_in,
    b_in,
    c_in,
    dt_in,
    conv_x,
    conv_b,
    conv_c,
    bias_ref,
    decay_ref,
    gain_ref,
    skip_ref,
    windows_ref,
    doclen_ref,
    attn_ref,
    mamba_ref,
    asum_ref,
    msum_ref,
    qbuf,
    kv,
    xbc,
    dtbuf,
    xc,
    bcbuf,
    full,
    inflow_ref,
    gapbuf,
    colbuf,
    cumt,
    deltat,
    crossm,
    state,
    gstate,
    fac,
    gfac,
    fexp,
    ret,
    incf,
    incoming,
    sums,
    a_send,
    a_recv,
    kv_send,
    kv_recv,
    tail_sem,
    st_send,
    st_recv,
    f_send,
    f_recv,
    r_send,
    r_recv,
    c_send,
    c_recv,
):
    me = lax.axis_index("seq")
    mt = lax.axis_index("tensor")
    piece = q_in.shape[0]
    rows = piece * T
    qw, kw, xw = q_in.shape[1] // T, k_in.shape[1] // T, x_in.shape[1] // T
    bw = b_in.shape[1] // T
    heads = xw // MP
    groups = bw // MN
    per_group = heads // groups
    qheads = qw // HEAD_SIZE
    holders = gstate.shape[0] and state.shape[0] // gstate.shape[1]
    stride = S // holders
    srows = gstate.shape[1]

    barrier = pltpu.get_barrier_semaphore()
    for d in range(1, T):
        pl.semaphore_signal(
            barrier, inc=1, device_id={"tensor": lax.rem(mt + d, T)},
            device_id_type=pl.DeviceIdType.MESH,
        )

    def greet(d, carry):
        pl.semaphore_signal(
            barrier, inc=1, device_id={"seq": lax.rem(me + d, S)},
            device_id_type=pl.DeviceIdType.MESH,
        )
        return carry

    lax.fori_loop(1, S, greet, 0)
    pl.semaphore_wait(barrier, T - 1 + S - 1)

    base = me * rows

    def dst_of(a, source):
        if a == 0:
            return kv.at[pl.ds(pl.multiple_of(base + source * piece, piece), piece), pl.ds(0, kw)]
        if a == 1:
            return kv.at[pl.ds(pl.multiple_of(base + source * piece, piece), piece), pl.ds(kw, kw)]
        ext = pl.ds(pl.multiple_of(TAIL + source * piece, TAIL), piece)
        if a == 2:
            return dtbuf.at[pl.ds(pl.multiple_of(source * piece, piece), piece), :]
        if a == 3:
            return xbc.at[ext, pl.ds(xw, bw)]
        if a == 4:
            return xbc.at[ext, pl.ds(xw + bw, bw)]
        if a == 5:
            return xbc.at[ext, pl.ds(0, xw)]
        return qbuf.at[pl.ds(pl.multiple_of(source * piece, piece), piece), :]

    ins = (k_in, v_in, dt_in, b_in, c_in, x_in, q_in)
    widths = (kw, kw, None, bw, bw, xw, qw)

    def src_of(a, target):
        if widths[a] is None:
            return ins[a].at[:, :]
        w = widths[a]
        return ins[a].at[:, pl.ds(pl.multiple_of(target * w, w), w)]

    def a2a_send(a, d):
        target = lax.rem(mt + d, T)
        return rdma(src_of(a, target), dst_of(a, mt), a_send.at[a, d], a_recv.at[a, d], "tensor", target)

    def a2a_local(a):
        return pltpu.make_async_copy(src_of(a, mt), dst_of(a, mt), a_recv.at[a, 0])

    def a2a_wait(a):
        a2a_local(a).wait()
        for d in range(1, T):
            source = lax.rem(mt + T - d, T)
            rdma(
                src_of(a, mt), dst_of(a, source), a_send.at[a, d], a_recv.at[a, d], "tensor", source
            ).wait_recv()

    for a in range(7):
        for d in range(1, T):
            a2a_send(a, d).start()
        a2a_local(a).start()

    starts = []
    running = jnp.int32(0)
    for i in range(doclen_ref.shape[0]):
        starts.append(running)
        running = running + doclen_ref[i]

    keys = S * rows
    key_chunk = min(keys, 1024)
    n_chunks = keys // key_chunk

    def gap_chunk(c, carry):
        t = base + iota((rows, key_chunk), 0)
        s = c * key_chunk + iota((rows, key_chunk), 1)
        dq = doc_of(base + iota((rows, 1), 0), starts)
        dk = doc_of(c * key_chunk + iota((1, key_chunk), 1), starts)
        gap = t - s
        ok = (gap >= 0) & (dq == dk)
        gapbuf[:, pl.ds(pl.multiple_of(c * key_chunk, key_chunk), key_chunk)] = jnp.where(
            ok, gap, jnp.int32(1 << 30)
        )
        return carry

    lax.fori_loop(0, n_chunks, gap_chunk, 0)

    a2a_wait(0)
    a2a_wait(1)

    def kv_block(owner):
        return kv.at[pl.ds(pl.multiple_of(owner * rows, rows), rows), :]

    def kv_copy(d, owner, peer):
        return rdma(kv_block(owner), kv_block(owner), kv_send.at[d], kv_recv.at[d], "seq", peer)

    def kv_start(d, carry):
        kv_copy(d, me, lax.rem(me + d, S)).start()
        return carry

    lax.fori_loop(1, S, kv_start, 0)

    a2a_wait(2)
    hot = (iota((LANES, heads), 0) == iota((LANES, heads), 1) + mt * heads).astype(BF16)
    dt = mm(dtbuf[...], hot)
    v = dt + bias_ref[...]
    delta = jnp.maximum(v, 0.0) + jnp.log1p(jnp.exp(-jnp.abs(v)))
    logd = -delta * decay_ref[...]
    lower = (iota((rows, rows), 0) >= iota((rows, rows), 1)).astype(BF16)
    cum = sum(mm(lower, p) for p in parts3(logd))
    eye = (iota((heads, heads), 0) == iota((heads, heads), 1)).astype(BF16)
    cumt[...] = sum(mm_t(eye, p) for p in parts3(cum))
    deltat[...] = sum(mm_t(eye, p) for p in parts3(delta))
    for i in range(heads // 2):
        colbuf[i, :, :] = cum[:, 2 * i : 2 * i + 2]
    docs = doc_of(base + iota((rows, 1), 0), starts)
    docs_row = doc_of(base + iota((1, rows), 1), starts)
    last_doc = doc_of(base + rows - 1 + jnp.zeros((1, 1), jnp.int32), starts)
    prior_doc = doc_of(base - 1 + jnp.zeros((1, 1), jnp.int32), starts)
    ending = cum[rows - 1 : rows, :]
    to_end = jnp.where(docs == last_doc, jnp.exp(ending - cum), 0.0) * delta
    factor = jnp.where(prior_doc == last_doc, jnp.exp(ending), 0.0)
    fac[...] = jnp.broadcast_to(factor, fac.shape)
    inflow = jnp.where(docs == prior_doc, jnp.exp(cum), 0.0)
    te = parts3(to_end)
    inf = parts3(inflow)

    a2a_wait(3)
    a2a_wait(4)
    a2a_wait(5)

    def tail_copy(peer):
        return rdma(
            xbc.at[pl.ds(rows, TAIL), :], xbc.at[pl.ds(0, TAIL), :],
            tail_sem.at[0], tail_sem.at[1], "seq", peer,
        )

    @pl.when(me < S - 1)
    def _():
        tail_copy(lax.rem(me + 1, S)).start()

    @pl.when(me > 0)
    def _():
        tail_copy(lax.rem(me + S - 1, S)).wait_recv()

    @pl.when(me == 0)
    def _():
        xbc[pl.ds(0, TAIL), :] = jnp.zeros((TAIL, xbc.shape[1]), BF16)

    width = 256 if xw % 256 == 0 and bw % 256 == 0 else 128
    pos = base + iota((rows, 1), 0)
    keeps = []
    for j in range(KC):
        same = (doc_of(pos - j, starts) == docs) & (pos - j >= 0)
        keeps.append(jnp.broadcast_to(same.astype(F32), (rows, width)))

    def conv(lane, taps, tap_lane):
        xe = xbc[:, pl.ds(lane, width)].astype(F32)
        tp = taps[:, pl.ds(tap_lane, width)].astype(F32)
        u = tp[0:1] * xe[TAIL : TAIL + rows]
        for j in range(1, KC):
            u = u + (tp[j : j + 1] * xe[TAIL - j : TAIL - j + rows]) * keeps[j]
        return (u / (1.0 + jnp.exp(-u))).astype(BF16)

    for i in range(bw // width):
        bcbuf[:, i * width : (i + 1) * width] = conv(xw + i * width, conv_b, i * width)
        bcbuf[:, bw + i * width : bw + (i + 1) * width] = conv(
            xw + bw + i * width, conv_c, i * width
        )

    causal = (iota((rows, rows), 0) >= iota((rows, rows), 1)) & (docs == docs_row)
    for g in range(groups):
        bg = bcbuf[:, g * MN : (g + 1) * MN]
        cg = bcbuf[:, bw + g * MN : bw + (g + 1) * MN]
        crossm[g] = jnp.where(causal, mm_t(cg, bg), 0.0)

    for g in range(groups):
        bt = bcbuf[:, g * MN : (g + 1) * MN].astype(F32).T.astype(BF16)
        gw = per_group * MP

        def stretch(i, carry, g=g, gw=gw, bt=bt):
            lane = pl.multiple_of(g * gw + i * width, width)
            out = conv(lane, conv_x, lane)
            xc[:, pl.ds(lane, width)] = out
            spread = (
                iota((heads, width), 0) == (lane + iota((heads, width), 1)) // MP
            ).astype(BF16)
            to_end_x = mm(te[0], spread) + mm(te[1], spread) + mm(te[2], spread)
            inflow_ref[:, pl.ds(lane, width)] = (
                mm(inf[0], spread) + mm(inf[1], spread) + mm(inf[2], spread)
            )
            weighted = (to_end_x * out.astype(F32)).astype(BF16)
            state[:, pl.ds(lane, width)] = mm(bt, weighted).astype(BF16)
            return carry

        lax.fori_loop(0, gw // width, stretch, 0)

    def st_copy(d, holder, owner, peer):
        return rdma(
            state.at[pl.ds(pl.multiple_of(holder * srows, srows), srows), :],
            gstate.at[owner], st_send.at[d], st_recv.at[d], "seq", peer,
        )

    def f_copy(d, owner, peer):
        return rdma(fac, gfac.at[owner], f_send.at[d], f_recv.at[d], "seq", peer)

    def st_local():
        return pltpu.make_async_copy(
            state.at[pl.ds(pl.multiple_of((me // stride) * srows, srows), srows), :],
            gstate.at[me], st_recv.at[0],
        )

    def st_start(d, carry):
        peer = lax.rem(me + d, S)

        @pl.when(lax.rem(peer, stride) == 0)
        def _():
            st_copy(d, peer // stride, me, peer).start()
            f_copy(d, me, peer).start()

        return carry

    lax.fori_loop(1, S, st_start, 0)
    is_holder = lax.rem(me, stride) == 0

    @pl.when(is_holder)
    def _():
        st_local().start()
        gfac[me] = fac[...]

    half = iota((1, 2 * MP), 1) < MP

    def intra(i, carry):
        lane = pl.multiple_of(i * 2 * MP, 2 * MP)
        cols = colbuf[i]
        cross = crossm[(2 * i) // per_group]
        mixes = []
        for k in range(2):
            gap = cols[:, k : k + 1] - cumt[pl.ds(2 * i + k, 1), :]
            w = jnp.exp(jnp.minimum(gap, 0.0)) * deltat[pl.ds(2 * i + k, 1), :]
            mixes.append((w * cross).astype(BF16))
        xp = xc[:, pl.ds(lane, 2 * MP)]
        zero = jnp.zeros_like(xp)
        halves = jnp.broadcast_to(half, xp.shape)
        stacked = jnp.concatenate(
            [jnp.where(halves, xp, zero), jnp.where(halves, zero, xp)], axis=0
        )
        skip = jnp.where(half, skip_ref[2 * i], skip_ref[2 * i + 1])
        full[:, pl.ds(lane, 2 * MP)] = (
            mm(jnp.concatenate(mixes, axis=1), stacked) + skip * xp.astype(F32)
        )
        return carry

    lax.fori_loop(0, heads // 2, intra, 0)

    def ret_copy(d, target, holder, peer):
        return rdma(
            ret.at[target],
            incoming.at[pl.ds(pl.multiple_of(holder * srows, srows), srows), :],
            r_send.at[d], r_recv.at[d], "seq", peer,
        )

    def ret_local():
        return pltpu.make_async_copy(
            ret.at[me],
            incoming.at[pl.ds(pl.multiple_of((me // stride) * srows, srows), srows), :],
            r_recv.at[0],
        )

    @pl.when(is_holder)
    def _():
        st_local().wait()

        def arrive(d, carry):
            owner = lax.rem(me + S - d, S)
            st_copy(d, me // stride, owner, owner).wait_recv()
            f_copy(d, owner, owner).wait_recv()
            return carry

        lax.fori_loop(1, S, arrive, 0)
        spread = (iota((heads, xw), 0) == iota((heads, xw), 1) // MP).astype(BF16)
        fp = parts3(gfac[...].reshape(S * 8, heads))
        fexp[...] = (mm(fp[0], spread) + mm(fp[1], spread) + mm(fp[2], spread)).reshape(
            S, 8, xw
        )
        incf[...] = jnp.zeros_like(incf)

        def scan(k, carry):
            now = incf[...]
            ret[k] = now.astype(BF16)
            incf[...] = fexp[k][0:1, :] * now + gstate[k].astype(F32)
            return carry

        lax.fori_loop(0, S, scan, 0)
        ret_local().start()

        def give(d, carry):
            peer = lax.rem(me + d, S)
            ret_copy(d, peer, me // stride, peer).start()
            return carry

        lax.fori_loop(1, S, give, 0)

    a2a_wait(6)

    def kv_wait(d, carry):
        owner = lax.rem(me + S - d, S)
        kv_copy(d, owner, owner).wait_recv()
        return carry

    lax.fori_loop(1, S, kv_wait, 0)

    to_exp2 = math.log2(math.e) / math.sqrt(HEAD_SIZE)
    width_of_group = qheads // (kw // HEAD_SIZE)

    def attend(i, carry):
        lane = pl.multiple_of(i * 2 * HEAD_SIZE, 2 * HEAD_SIZE)
        q2 = jnp.concatenate(
            [qbuf[:, pl.ds(lane, HEAD_SIZE)],
             qbuf[:, pl.ds(pl.multiple_of(lane + HEAD_SIZE, HEAD_SIZE), HEAD_SIZE)]], axis=0
        )
        g = (2 * i) // width_of_group
        klane = pl.multiple_of(g * HEAD_SIZE, HEAD_SIZE)
        vlane = pl.multiple_of(kw + g * HEAD_SIZE, HEAD_SIZE)
        wins = [windows_ref[mt * qheads + 2 * i + k] for k in range(2)]

        def piece_of(c, old):
            ks = pl.ds(pl.multiple_of(c * key_chunk, key_chunk), key_chunk)
            s = mm_t(q2, kv[ks, pl.ds(klane, HEAD_SIZE)])
            gap = gapbuf[:, ks]
            s = jnp.concatenate(
                [jnp.where(gap < wins[k], s[k * rows : (k + 1) * rows], NEG_LARGE)
                 for k in range(2)], axis=0
            )
            top = jnp.max(s, axis=1, keepdims=True)
            if old is not None:
                top = jnp.maximum(top, old[0])
            w = jnp.exp2((s - top) * to_exp2)
            total = jnp.sum(w, axis=1, keepdims=True)
            acc = mm(w.astype(BF16), kv[ks, pl.ds(vlane, HEAD_SIZE)])
            if old is not None:
                shrink = jnp.exp2((old[0] - top) * to_exp2)
                total = total + shrink * old[1]
                acc = acc + shrink * old[2]
            return top, total, acc

        if n_chunks == 1:
            top, total, acc = piece_of(0, None)
        else:
            top, total, acc = lax.fori_loop(
                0, n_chunks, piece_of,
                (jnp.full((2 * rows, 1), NEG_LARGE, F32), jnp.zeros((2 * rows, 1), F32),
                 jnp.zeros((2 * rows, HEAD_SIZE), F32)),
            )
        out = (acc / total).astype(BF16)
        for k in range(2):
            o = out[k * rows : (k + 1) * rows]
            at = pl.ds(pl.multiple_of(lane + k * HEAD_SIZE, HEAD_SIZE), HEAD_SIZE)
            attn_ref[:, at] = o
            sums[me, :, at] = jnp.sum(o.astype(F32), axis=0, keepdims=True)
        return carry

    lax.fori_loop(0, qheads // 2, attend, 0)

    def collect(h, carry):
        @pl.when(h * stride != me)
        def _():
            peer = h * stride
            d = lax.rem(me - peer + S, S)
            ret_copy(d, me, h, peer).wait_recv()

        return carry

    lax.fori_loop(0, holders, collect, 0)

    @pl.when(is_holder)
    def _():
        ret_local().wait()

    pair = 2 * MP
    ones = (iota((pair, pair), 0) // MP == iota((pair, pair), 1) // MP).astype(BF16)

    def finish(i, carry):
        lane = pl.multiple_of(i * pair, pair)
        g = (2 * i) // per_group
        cg = bcbuf[:, pl.ds(pl.multiple_of(bw + g * MN, MN), MN)]
        entering = mm(cg, incoming[:, pl.ds(lane, pair)])
        y = full[:, pl.ds(lane, pair)] + entering * inflow_ref[:, pl.ds(lane, pair)]
        p = parts3(y * y)
        mean = (mm(p[0], ones) + mm(p[1], ones) + mm(p[2], ones)) * (1.0 / MP)
        o = (y * lax.rsqrt(mean + EPS_NORM) * gain_ref[:, pl.ds(lane, pair)]).astype(BF16)
        mamba_ref[:, pl.ds(lane, pair)] = o
        sums[me, :, pl.ds(pl.multiple_of(qw + lane, pair), pair)] = jnp.sum(
            o.astype(F32), axis=0, keepdims=True
        )
        return carry

    lax.fori_loop(0, heads // 2, finish, 0)

    def sum_copy(d, owner, peer):
        return rdma(sums.at[owner], sums.at[owner], c_send.at[d], c_recv.at[d], "seq", peer)

    def sum_start(d, carry):
        sum_copy(d, me, lax.rem(me + d, S)).start()
        return carry

    lax.fori_loop(1, S, sum_start, 0)

    for a in range(7):
        for d in range(1, T):
            a2a_send(a, d).wait_send()

    @pl.when(me < S - 1)
    def _():
        tail_copy(lax.rem(me + 1, S)).wait_send()

    def drain(d, carry):
        peer = lax.rem(me + d, S)
        kv_copy(d, me, peer).wait_send()

        @pl.when(lax.rem(peer, stride) == 0)
        def _():
            st_copy(d, peer // stride, me, peer).wait_send()
            f_copy(d, me, peer).wait_send()

        @pl.when(is_holder)
        def _():
            ret_copy(d, peer, me // stride, peer).wait_send()

        return carry

    lax.fori_loop(1, S, drain, 0)

    def sum_wait(d, carry):
        owner = lax.rem(me + S - d, S)
        sum_copy(d, owner, owner).wait_recv()
        sum_copy(d, me, lax.rem(me + d, S)).wait_send()
        return carry

    lax.fori_loop(1, S, sum_wait, 0)

    def add(k, total):
        return total + sums[k]

    total = lax.fori_loop(0, S, add, jnp.zeros((1, sums.shape[2]), F32))
    asum_ref[...] = total[:, :qw]
    msum_ref[...] = total[:, qw:]


def local(
    S,
    T,
    queries,
    keys,
    values,
    mamba_x,
    mamba_b,
    mamba_c,
    mamba_dt,
    conv_x,
    conv_b,
    conv_c,
    dt_bias,
    decay_rate,
    skip_gain,
    norm_gain,
    windows,
    doc_lengths,
):
    rows = queries.shape[0] * T
    qw, kw, xw, bw = (a.shape[1] // T for a in (queries, keys, mamba_x, mamba_b))
    heads = xw // MP
    holders = min(S, MN // 16)
    srows = MN // holders
    vmem = pl.BlockSpec(memory_space=pltpu.VMEM)
    smem = pl.BlockSpec(memory_space=pltpu.SMEM)
    dma = pltpu.SemaphoreType.DMA
    attn, mamba, asum, msum = pl.pallas_call(
        functools.partial(kernel, S, T),
        out_shape=(
            jax.ShapeDtypeStruct((rows, qw), BF16),
            jax.ShapeDtypeStruct((rows, xw), BF16),
            jax.ShapeDtypeStruct((1, qw), F32),
            jax.ShapeDtypeStruct((1, xw), F32),
        ),
        in_specs=[vmem] * 13 + [smem] * 3,
        out_specs=(vmem,) * 4,
        scratch_shapes=[
            pltpu.VMEM((rows, qw), BF16),
            pltpu.VMEM((S * rows, 2 * kw), BF16),
            pltpu.VMEM((TAIL + rows, xw + 2 * bw), BF16),
            pltpu.VMEM((rows, mamba_dt.shape[1]), BF16),
            pltpu.VMEM((rows, xw), BF16),
            pltpu.VMEM((rows, 2 * bw), BF16),
            pltpu.VMEM((rows, xw), F32),
            pltpu.VMEM((rows, xw), F32),
            pltpu.VMEM((rows, S * rows), jnp.int32),
            pltpu.VMEM((heads // 2, rows, 2), F32),
            pltpu.VMEM((heads, rows), F32),
            pltpu.VMEM((heads, rows), F32),
            pltpu.VMEM((bw // MN, rows, rows), F32),
            pltpu.VMEM((MN, xw), BF16),
            pltpu.VMEM((S, srows, xw), BF16),
            pltpu.VMEM((8, heads), F32),
            pltpu.VMEM((S, 8, heads), F32),
            pltpu.VMEM((S, 8, xw), F32),
            pltpu.VMEM((S, srows, xw), BF16),
            pltpu.VMEM((srows, xw), F32),
            pltpu.VMEM((MN, xw), BF16),
            pltpu.VMEM((S, 1, qw + xw), F32),
            dma((7, T)),
            dma((7, T)),
            dma((S,)),
            dma((S,)),
            dma((2,)),
            dma((S,)),
            dma((S,)),
            dma((S,)),
            dma((S,)),
            dma((S,)),
            dma((S,)),
            dma((S,)),
            dma((S,)),
        ],
        compiler_params=pltpu.CompilerParams(
            collective_id=0, has_side_effects=True, vmem_limit_bytes=60 * 1024 * 1024
        ),
    )(
        queries, keys, values, mamba_x, mamba_b, mamba_c, mamba_dt, conv_x, conv_b, conv_c,
        dt_bias.reshape(1, -1), decay_rate.reshape(1, -1), norm_gain.reshape(1, -1),
        skip_gain, windows, doc_lengths,
    )
    return attn, mamba, asum.reshape(-1), msum.reshape(-1)


def solution(mesh):
    rows = P(("seq", "tensor"), None)
    return jax.shard_map(
        functools.partial(local, mesh.shape["seq"], mesh.shape["tensor"]),
        mesh=mesh,
        in_specs=(rows,) * 7 + (P(None, "tensor"),) * 3 + (P("tensor"),) * 4 + (P(), P()),
        out_specs=(P("seq", "tensor"), P("seq", "tensor"), P("tensor"), P("tensor")),
        check_vma=False,
    )
```

```python
import functools
import math

import jax
import jax.numpy as jnp
from jax import lax
from jax.experimental import pallas as pl
from jax.experimental.pallas import tpu as pltpu
from jax.sharding import PartitionSpec as P

HEAD_SIZE = 128
MP = 64
MN = 128
KC = 4
TAIL = 16
LANES = 128

NEG_LARGE = -1e30
EPS_NORM = 1e-05
F32 = jnp.float32
BF16 = jnp.bfloat16


def parts3(v):
    a = v.astype(BF16)
    r = v - a.astype(F32)
    b = r.astype(BF16)
    c = (r - b.astype(F32)).astype(BF16)
    return a, b, c


def mm(a, b):
    return jnp.dot(a, b, preferred_element_type=F32)


def mm_t(a, b):
    return lax.dot_general(a, b, (((1,), (1,)), ((), ())), preferred_element_type=F32)


def iota(shape, dim):
    return lax.broadcasted_iota(jnp.int32, shape, dim)


def doc_of(pos, starts):
    total = jnp.full(pos.shape, -1, jnp.int32)
    for s in starts:
        total = total + (pos >= s).astype(jnp.int32)
    return total


def rdma(src, dst, send, recv, axis, peer):
    return pltpu.make_async_remote_copy(
        src_ref=src,
        dst_ref=dst,
        send_sem=send,
        recv_sem=recv,
        device_id={axis: peer},
        device_id_type=pl.DeviceIdType.MESH,
    )


def kernel(
    S,
    T,
    q_in,
    k_in,
    v_in,
    x_in,
    b_in,
    c_in,
    dt_in,
    conv_x,
    conv_b,
    conv_c,
    bias_ref,
    decay_ref,
    gain_ref,
    skip_ref,
    windows_ref,
    doclen_ref,
    attn_ref,
    mamba_ref,
    asum_ref,
    msum_ref,
    qbuf,
    kv,
    xbc,
    dtbuf,
    xc,
    bcbuf,
    full,
    inflow_ref,
    gapbuf,
    colbuf,
    cumt,
    deltat,
    crossm,
    state,
    gstate,
    fac,
    gfac,
    fexp,
    ret,
    incoming,
    sums,
    a_send,
    a_recv,
    kv_send,
    kv_recv,
    tail_sem,
    st_send,
    st_recv,
    f_send,
    f_recv,
    r_send,
    r_recv,
    c_send,
    c_recv,
):
    me = lax.axis_index("seq")
    mt = lax.axis_index("tensor")
    piece = q_in.shape[0]
    rows = piece * T
    qw, kw, xw = q_in.shape[1] // T, k_in.shape[1] // T, x_in.shape[1] // T
    bw = b_in.shape[1] // T
    heads = xw // MP
    groups = bw // MN
    per_group = heads // groups
    qheads = qw // HEAD_SIZE
    holders = gstate.shape[0] and state.shape[0] // gstate.shape[1]
    stride = S // holders
    srows = gstate.shape[1]

    barrier = pltpu.get_barrier_semaphore()
    for d in range(1, T):
        pl.semaphore_signal(
            barrier, inc=1, device_id={"tensor": lax.rem(mt + d, T)},
            device_id_type=pl.DeviceIdType.MESH,
        )

    def greet(d, carry):
        pl.semaphore_signal(
            barrier, inc=1, device_id={"seq": lax.rem(me + d, S)},
            device_id_type=pl.DeviceIdType.MESH,
        )
        return carry

    lax.fori_loop(1, S, greet, 0)
    pl.semaphore_wait(barrier, T - 1 + S - 1)

    base = me * rows
    NP = st_send.shape[0]
    pw = xw // NP
    Q = 5 + NP

    def dst_of(a, source):
        if a == 0:
            return kv.at[pl.ds(pl.multiple_of(base + source * piece, piece), piece), pl.ds(0, kw)]
        if a == 1:
            return kv.at[pl.ds(pl.multiple_of(base + source * piece, piece), piece), pl.ds(kw, kw)]
        ext = pl.ds(pl.multiple_of(TAIL + source * piece, TAIL), piece)
        if a == 2:
            return dtbuf.at[pl.ds(pl.multiple_of(source * piece, piece), piece), :]
        if a == 3:
            return xbc.at[ext, pl.ds(xw, bw)]
        if a == 4:
            return xbc.at[ext, pl.ds(xw + bw, bw)]
        if a < 5 + NP:
            return xbc.at[ext, pl.ds((a - 5) * pw, pw)]
        return qbuf.at[pl.ds(pl.multiple_of(source * piece, piece), piece), :]

    ins = (k_in, v_in, dt_in, b_in, c_in) + (x_in,) * NP + (q_in,)
    widths = (kw, kw, None, bw, bw) + (xw,) * NP + (qw,)

    def src_of(a, target):
        if widths[a] is None:
            return ins[a].at[:, :]
        w = widths[a]
        if 5 <= a < Q:
            return x_in.at[:, pl.ds(pl.multiple_of(target * w + (a - 5) * pw, pw), pw)]
        return ins[a].at[:, pl.ds(pl.multiple_of(target * w, w), w)]

    def a2a_send(a, d):
        target = lax.rem(mt + d, T)
        return rdma(src_of(a, target), dst_of(a, mt), a_send.at[a, d], a_recv.at[a, d], "tensor", target)

    def a2a_local(a):
        return pltpu.make_async_copy(src_of(a, mt), dst_of(a, mt), a_recv.at[a, 0])

    def a2a_wait(a):
        a2a_local(a).wait()
        for d in range(1, T):
            source = lax.rem(mt + T - d, T)
            rdma(
                src_of(a, mt), dst_of(a, source), a_send.at[a, d], a_recv.at[a, d], "tensor", source
            ).wait_recv()

    low = mt < (T + 1) // 2
    order = []
    for e in range(T - 1):
        down = jnp.where(T - 1 - e > mt, T - 1 - e, T - 2 - e)
        up = jnp.where(e < mt, e, e + 1)
        order.append(lax.rem(jnp.where(low, down, up) - mt + T, T))
    for a in (2, 3, 4, 0, 1, *range(5, Q + 1)):
        for d in order:
            a2a_send(a, d).start()
        a2a_local(a).start()

    starts = []
    running = jnp.int32(0)
    for i in range(doclen_ref.shape[0]):
        starts.append(running)
        running = running + doclen_ref[i]

    keys = S * rows
    key_chunk = min(keys, 1024)
    n_chunks = keys // key_chunk

    def gap_chunk(c, carry):
        t = base + iota((rows, key_chunk), 0)
        s = c * key_chunk + iota((rows, key_chunk), 1)
        dq = doc_of(base + iota((rows, 1), 0), starts)
        dk = doc_of(c * key_chunk + iota((1, key_chunk), 1), starts)
        gap = t - s
        ok = (gap >= 0) & (dq == dk)
        gapbuf[:, pl.ds(pl.multiple_of(c * key_chunk, key_chunk), key_chunk)] = jnp.where(
            ok, gap, jnp.int32(1 << 30)
        )
        return carry

    lax.fori_loop(0, n_chunks, gap_chunk, 0)

    a2a_wait(2)
    hot = (iota((LANES, heads), 0) == iota((LANES, heads), 1) + mt * heads).astype(BF16)
    dt = mm(dtbuf[...], hot)
    v = dt + bias_ref[...]
    delta = jnp.maximum(v, 0.0) + jnp.log1p(jnp.exp(-jnp.abs(v)))
    logd = -delta * decay_ref[...]
    lower = (iota((rows, rows), 0) >= iota((rows, rows), 1)).astype(BF16)
    cum = sum(mm(lower, p) for p in parts3(logd))
    eye = (iota((heads, heads), 0) == iota((heads, heads), 1)).astype(BF16)
    cumt[...] = sum(mm_t(eye, p) for p in parts3(cum))
    deltat[...] = sum(mm_t(eye, p) for p in parts3(delta))
    for i in range(heads // 2):
        colbuf[i, :, :] = cum[:, 2 * i : 2 * i + 2]
    docs = doc_of(base + iota((rows, 1), 0), starts)
    docs_row = doc_of(base + iota((1, rows), 1), starts)
    last_doc = doc_of(base + rows - 1 + jnp.zeros((1, 1), jnp.int32), starts)
    prior_doc = doc_of(base - 1 + jnp.zeros((1, 1), jnp.int32), starts)
    ending = cum[rows - 1 : rows, :]
    to_end = jnp.where(docs == last_doc, jnp.exp(ending - cum), 0.0) * delta
    factor = jnp.where(prior_doc == last_doc, jnp.exp(ending), 0.0)
    fac[...] = jnp.broadcast_to(factor, fac.shape)
    inflow = jnp.where(docs == prior_doc, jnp.exp(cum), 0.0)
    te = parts3(to_end)[:2]
    inf = parts3(inflow)[:2]

    def f_copy(d, owner, peer):
        return rdma(fac, gfac.at[owner], f_send.at[d], f_recv.at[d], "seq", peer)

    is_holder = lax.rem(me, stride) == 0

    def f_start(d, carry):
        peer = lax.rem(me + d, S)

        @pl.when(lax.rem(peer, stride) == 0)
        def _():
            f_copy(d, me, peer).start()

        return carry

    lax.fori_loop(1, S, f_start, 0)
    gfac[me] = fac[...]

    a2a_wait(3)
    a2a_wait(4)

    def tail_copy(p, peer):
        lanes = pl.ds(p * pw, pw) if p < NP else pl.ds(xw, 2 * bw)
        return rdma(
            xbc.at[pl.ds(rows, TAIL), lanes], xbc.at[pl.ds(0, TAIL), lanes],
            tail_sem.at[p, 0], tail_sem.at[p, 1], "seq", peer,
        )

    def tail_start(p):
        @pl.when(me < S - 1)
        def _():
            tail_copy(p, lax.rem(me + 1, S)).start()

    def tail_wait(p):
        @pl.when(me > 0)
        def _():
            tail_copy(p, lax.rem(me + S - 1, S)).wait_recv()

    @pl.when(me == 0)
    def _():
        xbc[pl.ds(0, TAIL), :] = jnp.zeros((TAIL, xbc.shape[1]), BF16)

    tail_start(NP)

    a2a_wait(0)
    a2a_wait(1)

    twin = me + 1 - 2 * lax.rem(me, 2)

    def kv_block(owner):
        return kv.at[pl.ds(pl.multiple_of(owner * rows, rows), rows), :]

    def kv_copy(d, owner, peer):
        return rdma(kv_block(owner), kv_block(owner), kv_send.at[d], kv_recv.at[d], "seq", peer)

    def kv_start(e, carry):
        kv_copy(e, me, lax.rem(me + 2 * e, S)).start()
        return carry

    lax.fori_loop(1, S // 2, kv_start, 0)
    kv_copy(0, me, twin).start()

    @pl.when(is_holder)
    def _():
        def arrive(d, carry):
            owner = lax.rem(me + S - d, S)
            f_copy(d, owner, owner).wait_recv()
            return carry

        lax.fori_loop(1, S, arrive, 0)
        spread = (iota((heads, xw), 0) == iota((heads, xw), 1) // MP).astype(BF16)
        fp = parts3(gfac[...].reshape(S * 8, heads))
        fexp[...] = (mm(fp[0], spread) + mm(fp[1], spread) + mm(fp[2], spread)).reshape(
            S, 8, xw
        )

    tail_wait(NP)
    width = 256 if xw % 256 == 0 and bw % 256 == 0 else 128
    pos = base + iota((rows, 1), 0)
    keeps = []
    for j in range(KC):
        same = (doc_of(pos - j, starts) == docs) & (pos - j >= 0)
        keeps.append(jnp.broadcast_to(same.astype(F32), (rows, width)))

    def conv(lane, taps, tap_lane):
        xe = xbc[:, pl.ds(lane, width)].astype(F32)
        tp = taps[:, pl.ds(tap_lane, width)].astype(F32)
        u = tp[0:1] * xe[TAIL : TAIL + rows]
        for j in range(1, KC):
            u = u + (tp[j : j + 1] * xe[TAIL - j : TAIL - j + rows]) * keeps[j]
        return (u / (1.0 + jnp.exp(-u))).astype(BF16)

    for i in range(bw // width):
        bcbuf[:, i * width : (i + 1) * width] = conv(xw + i * width, conv_b, i * width)
        bcbuf[:, bw + i * width : bw + (i + 1) * width] = conv(
            xw + bw + i * width, conv_c, i * width
        )

    causal = (iota((rows, rows), 0) >= iota((rows, rows), 1)) & (docs == docs_row)
    for g in range(groups):
        bg = bcbuf[:, g * MN : (g + 1) * MN]
        cg = bcbuf[:, bw + g * MN : bw + (g + 1) * MN]
        crossm[g] = jnp.where(causal, mm_t(cg, bg), 0.0)

    bts = [
        bcbuf[:, g * MN : (g + 1) * MN].astype(F32).T.astype(BF16) for g in range(groups)
    ]
    gw = per_group * MP

    def stretch(lane):
        out = conv(lane, conv_x, lane)
        xc[:, lane : lane + width] = out
        spread = (
            iota((heads, width), 0) == (lane + iota((heads, width), 1)) // MP
        ).astype(BF16)
        inflow_ref[:, lane : lane + width] = mm(inf[0], spread) + mm(inf[1], spread)
        weighted = ((mm(te[0], spread) + mm(te[1], spread)) * out.astype(F32)).astype(BF16)
        state[:, lane : lane + width] = mm(bts[lane // gw], weighted).astype(BF16)

    def st_copy(p, d, holder, owner, peer):
        lanes = pl.ds(p * pw, pw)
        return rdma(
            state.at[pl.ds(pl.multiple_of(holder * srows, srows), srows), lanes],
            gstate.at[owner, :, lanes], st_send.at[p, d], st_recv.at[p, d], "seq", peer,
        )

    def st_local(p):
        lanes = pl.ds(p * pw, pw)
        return pltpu.make_async_copy(
            state.at[pl.ds(pl.multiple_of((me // stride) * srows, srows), srows), lanes],
            gstate.at[me, :, lanes], st_recv.at[p, 0],
        )

    def st_issue(p):
        def st_start(d, carry):
            peer = lax.rem(me + d, S)

            @pl.when(lax.rem(peer, stride) == 0)
            def _():
                st_copy(p, d, peer // stride, me, peer).start()

            return carry

        lax.fori_loop(1, S, st_start, 0)

        @pl.when(is_holder)
        def _():
            st_local(p).start()

    half = iota((1, 2 * MP), 1) < MP

    def intra(i, carry):
        lane = pl.multiple_of(i * 2 * MP, 2 * MP)
        cols = colbuf[i]
        cross = crossm[(2 * i) // per_group]
        mixes = []
        for k in range(2):
            gap = cols[:, k : k + 1] - cumt[pl.ds(2 * i + k, 1), :]
            w = jnp.exp(jnp.minimum(gap, 0.0)) * deltat[pl.ds(2 * i + k, 1), :]
            mixes.append((w * cross).astype(BF16))
        xp = xc[:, pl.ds(lane, 2 * MP)]
        zero = jnp.zeros_like(xp)
        halves = jnp.broadcast_to(half, xp.shape)
        stacked = jnp.concatenate(
            [jnp.where(halves, xp, zero), jnp.where(halves, zero, xp)], axis=0
        )
        skip = jnp.where(half, skip_ref[2 * i], skip_ref[2 * i + 1])
        full[:, pl.ds(lane, 2 * MP)] = (
            mm(jnp.concatenate(mixes, axis=1), stacked) + skip * xp.astype(F32)
        )
        return carry

    pairs = heads // 2 // NP

    def intra_piece(p):
        lax.fori_loop(p * pairs, (p + 1) * pairs, intra, 0, unroll=2)

    for p in range(NP):
        a2a_wait(5 + p)
        tail_start(p)
        if p > 0:
            intra_piece(p - 1)
        tail_wait(p)
        for i in range(pw // width):
            stretch(p * pw + i * width)
        st_issue(p)
    intra_piece(NP - 1)

    def kv_pass(e, carry):
        owner = lax.rem(me + S - 2 * e, S)
        kv_copy(e, owner, owner).wait_recv()
        kv_copy(S // 2 + e, owner, twin).start()
        return carry

    lax.fori_loop(1, S // 2, kv_pass, 0)

    def ret_copy(p, d, target, holder, peer):
        lanes = pl.ds(p * pw, pw)
        return rdma(
            ret.at[target, :, lanes],
            incoming.at[pl.ds(pl.multiple_of(holder * srows, srows), srows), lanes],
            r_send.at[p, d], r_recv.at[p, d], "seq", peer,
        )

    def ret_local(p):
        lanes = pl.ds(p * pw, pw)
        return pltpu.make_async_copy(
            ret.at[me, :, lanes],
            incoming.at[pl.ds(pl.multiple_of((me // stride) * srows, srows), srows), lanes],
            r_recv.at[p, 0],
        )

    def prefix_piece(p):
        lanes = slice(p * pw, (p + 1) * pw)

        @pl.when(is_holder)
        def _():
            st_local(p).wait()

            def arrive(d, carry):
                owner = lax.rem(me + S - d, S)
                st_copy(p, d, me // stride, owner, owner).wait_recv()
                return carry

            lax.fori_loop(1, S, arrive, 0)

            def scan(k, now):
                ret[k, :, lanes] = now.astype(BF16)
                return fexp[k, 0:1, lanes] * now + gstate[k, :, lanes].astype(F32)

            lax.fori_loop(0, S, scan, jnp.zeros((srows, pw), F32))
            ret_local(p).start()

            def give(d, carry):
                peer = lax.rem(me + d, S)
                ret_copy(p, d, peer, me // stride, peer).start()
                return carry

            lax.fori_loop(1, S, give, 0)

    for p in range(NP):
        prefix_piece(p)

    a2a_wait(Q)

    def kv_wait(e, carry):
        kv_copy(S // 2 + e, lax.rem(twin + S - 2 * e, S), twin).wait_recv()
        return carry

    lax.fori_loop(1, S // 2, kv_wait, 0)
    kv_copy(0, twin, twin).wait_recv()

    to_exp2 = math.log2(math.e) / math.sqrt(HEAD_SIZE)
    width_of_group = qheads // (kw // HEAD_SIZE)

    def attend(i, carry):
        lane = pl.multiple_of(i * 2 * HEAD_SIZE, 2 * HEAD_SIZE)
        q2 = jnp.concatenate(
            [qbuf[:, pl.ds(lane, HEAD_SIZE)],
             qbuf[:, pl.ds(pl.multiple_of(lane + HEAD_SIZE, HEAD_SIZE), HEAD_SIZE)]], axis=0
        )
        g = (2 * i) // width_of_group
        klane = pl.multiple_of(g * HEAD_SIZE, HEAD_SIZE)
        vlane = pl.multiple_of(kw + g * HEAD_SIZE, HEAD_SIZE)
        wins = [windows_ref[mt * qheads + 2 * i + k] for k in range(2)]

        def piece_of(c, old):
            ks = pl.ds(pl.multiple_of(c * key_chunk, key_chunk), key_chunk)
            s = mm_t(q2, kv[ks, pl.ds(klane, HEAD_SIZE)])
            gap = gapbuf[:, ks]
            s = jnp.concatenate(
                [jnp.where(gap < wins[k], s[k * rows : (k + 1) * rows], NEG_LARGE)
                 for k in range(2)], axis=0
            )
            top = jnp.max(s, axis=1, keepdims=True)
            if old is not None:
                top = jnp.maximum(top, old[0])
            w = jnp.exp2((s - top) * to_exp2)
            total = jnp.sum(w, axis=1, keepdims=True)
            acc = mm(w.astype(BF16), kv[ks, pl.ds(vlane, HEAD_SIZE)])
            if old is not None:
                shrink = jnp.exp2((old[0] - top) * to_exp2)
                total = total + shrink * old[1]
                acc = acc + shrink * old[2]
            return top, total, acc

        if n_chunks == 1:
            top, total, acc = piece_of(0, None)
        else:
            top, total, acc = lax.fori_loop(
                0, n_chunks, piece_of,
                (jnp.full((2 * rows, 1), NEG_LARGE, F32), jnp.zeros((2 * rows, 1), F32),
                 jnp.zeros((2 * rows, HEAD_SIZE), F32)),
            )
        out = (acc / total).astype(BF16)
        for k in range(2):
            o = out[k * rows : (k + 1) * rows]
            at = pl.ds(pl.multiple_of(lane + k * HEAD_SIZE, HEAD_SIZE), HEAD_SIZE)
            attn_ref[:, at] = o
            sums[me, :, at] = jnp.sum(o.astype(F32), axis=0, keepdims=True)
        return carry

    lax.fori_loop(0, qheads // 2, attend, 0)

    def collect_piece(p):
        def collect(h, carry):
            @pl.when(h * stride != me)
            def _():
                peer = h * stride
                d = lax.rem(me - peer + S, S)
                ret_copy(p, d, me, h, peer).wait_recv()

            return carry

        lax.fori_loop(0, holders, collect, 0)

        @pl.when(is_holder)
        def _():
            ret_local(p).wait()

    pair = 2 * MP
    ones = (iota((pair, pair), 0) // MP == iota((pair, pair), 1) // MP).astype(BF16)

    def finish(i, carry):
        lane = pl.multiple_of(i * pair, pair)
        g = (2 * i) // per_group
        cg = bcbuf[:, pl.ds(pl.multiple_of(bw + g * MN, MN), MN)]
        entering = mm(cg, incoming[:, pl.ds(lane, pair)])
        y = full[:, pl.ds(lane, pair)] + entering * inflow_ref[:, pl.ds(lane, pair)]
        p = parts3(y * y)
        mean = (mm(p[0], ones) + mm(p[1], ones)) * (1.0 / MP)
        o = (y * lax.rsqrt(mean + EPS_NORM) * gain_ref[:, pl.ds(lane, pair)]).astype(BF16)
        mamba_ref[:, pl.ds(lane, pair)] = o
        sums[me, :, pl.ds(pl.multiple_of(qw + lane, pair), pair)] = jnp.sum(
            o.astype(F32), axis=0, keepdims=True
        )
        return carry

    for p in range(NP):
        collect_piece(p)
        lax.fori_loop(p * pairs, (p + 1) * pairs, finish, 0, unroll=2)

    def sum_copy(d, owner, peer):
        return rdma(sums.at[owner], sums.at[owner], c_send.at[d], c_recv.at[d], "seq", peer)

    def sum_start(d, carry):
        sum_copy(d, me, lax.rem(me + d, S)).start()
        return carry

    lax.fori_loop(1, S, sum_start, 0)

    for a in range(Q + 1):
        for d in range(1, T):
            a2a_send(a, d).wait_send()

    @pl.when(me < S - 1)
    def _():
        for p in range(NP + 1):
            tail_copy(p, lax.rem(me + 1, S)).wait_send()

    def drain(d, carry):
        peer = lax.rem(me + d, S)

        @pl.when(lax.rem(peer, stride) == 0)
        def _():
            for p in range(NP):
                st_copy(p, d, peer // stride, me, peer).wait_send()
            f_copy(d, me, peer).wait_send()

        @pl.when(is_holder)
        def _():
            for p in range(NP):
                ret_copy(p, d, peer, me // stride, peer).wait_send()

        return carry

    lax.fori_loop(1, S, drain, 0)

    def kv_drain(e, carry):
        kv_copy(e, me, lax.rem(me + 2 * e, S)).wait_send()
        kv_copy(S // 2 + e, lax.rem(me + S - 2 * e, S), twin).wait_send()
        return carry

    lax.fori_loop(1, S // 2, kv_drain, 0)
    kv_copy(0, me, twin).wait_send()

    def sum_wait(d, carry):
        owner = lax.rem(me + S - d, S)
        sum_copy(d, owner, owner).wait_recv()
        sum_copy(d, me, lax.rem(me + d, S)).wait_send()
        return carry

    lax.fori_loop(1, S, sum_wait, 0)

    def add(k, total):
        return total + sums[k]

    total = lax.fori_loop(0, S, add, jnp.zeros((1, sums.shape[2]), F32))
    asum_ref[...] = total[:, :qw]
    msum_ref[...] = total[:, qw:]


def local(
    S,
    T,
    queries,
    keys,
    values,
    mamba_x,
    mamba_b,
    mamba_c,
    mamba_dt,
    conv_x,
    conv_b,
    conv_c,
    dt_bias,
    decay_rate,
    skip_gain,
    norm_gain,
    windows,
    doc_lengths,
):
    rows = queries.shape[0] * T
    qw, kw, xw, bw = (a.shape[1] // T for a in (queries, keys, mamba_x, mamba_b))
    heads = xw // MP
    holders = min(S, MN // 16)
    srows = MN // holders
    pieces = xw // 512 if xw % 512 == 0 else 1
    vmem = pl.BlockSpec(memory_space=pltpu.VMEM)
    smem = pl.BlockSpec(memory_space=pltpu.SMEM)
    dma = pltpu.SemaphoreType.DMA
    attn, mamba, asum, msum = pl.pallas_call(
        functools.partial(kernel, S, T),
        out_shape=(
            pltpu.VMEM((rows, qw), BF16),
            pltpu.VMEM((rows, xw), BF16),
            pltpu.VMEM((1, qw), F32),
            pltpu.VMEM((1, xw), F32),
        ),
        in_specs=[vmem] * 13 + [smem] * 3,
        out_specs=(vmem,) * 4,
        scratch_shapes=[
            pltpu.VMEM((rows, qw), BF16),
            pltpu.VMEM((S * rows, 2 * kw), BF16),
            pltpu.VMEM((TAIL + rows, xw + 2 * bw), BF16),
            pltpu.VMEM((rows, mamba_dt.shape[1]), BF16),
            pltpu.VMEM((rows, xw), BF16),
            pltpu.VMEM((rows, 2 * bw), BF16),
            pltpu.VMEM((rows, xw), F32),
            pltpu.VMEM((rows, xw), F32),
            pltpu.VMEM((rows, S * rows), jnp.int32),
            pltpu.VMEM((heads // 2, rows, 2), F32),
            pltpu.VMEM((heads, rows), F32),
            pltpu.VMEM((heads, rows), F32),
            pltpu.VMEM((bw // MN, rows, rows), F32),
            pltpu.VMEM((MN, xw), BF16),
            pltpu.VMEM((S, srows, xw), BF16),
            pltpu.VMEM((8, heads), F32),
            pltpu.VMEM((S, 8, heads), F32),
            pltpu.VMEM((S, 8, xw), F32),
            pltpu.VMEM((S, srows, xw), BF16),
            pltpu.VMEM((MN, xw), BF16),
            pltpu.VMEM((S, 1, qw + xw), F32),
            dma((6 + pieces, T)),
            dma((6 + pieces, T)),
            dma((S,)),
            dma((S,)),
            dma((pieces + 1, 2)),
            dma((pieces, S)),
            dma((pieces, S)),
            dma((S,)),
            dma((S,)),
            dma((pieces, S)),
            dma((pieces, S)),
            dma((S,)),
            dma((S,)),
        ],
        compiler_params=pltpu.CompilerParams(
            collective_id=0, has_side_effects=True, vmem_limit_bytes=60 * 1024 * 1024
        ),
    )(
        queries, keys, values, mamba_x, mamba_b, mamba_c, mamba_dt, conv_x, conv_b, conv_c,
        dt_bias.reshape(1, -1), decay_rate.reshape(1, -1), norm_gain.reshape(1, -1),
        skip_gain, windows, doc_lengths,
    )
    return attn, mamba, asum.reshape(-1), msum.reshape(-1)


def solution(mesh):
    rows = P(("seq", "tensor"), None)
    return jax.shard_map(
        functools.partial(local, mesh.shape["seq"], mesh.shape["tensor"]),
        mesh=mesh,
        in_specs=(rows,) * 7 + (P(None, "tensor"),) * 3 + (P("tensor"),) * 4 + (P(), P()),
        out_specs=(P("seq", "tensor"), P("seq", "tensor"), P("tensor"), P("tensor")),
        check_vma=False,
    )
```
